32 devices in a mesh: rows: 4 (over y, x), tp: 8 (over z, core).
Axes of the slice: x: 2, y: 2, z: 4, core: 2. Of those that a mesh axis runs over, the one named last changes fastest.
Arguments:
- train_gate: float32 [3584, 14336], P('rows', 'tp'), may hold values from -0.125 to 0.125
- drift_gate: float32 [3584, 14336], P('rows', 'tp'), may hold values from -6 to 6
- spread_gate: float32 [3584, 14336], P('rows', 'tp'), may hold values from 0.1 to 10
- train_up: float32 [3584, 14336], P('rows', 'tp'), may hold values from -0.125 to 0.125
- drift_up: float32 [3584, 14336], P('rows', 'tp'), may hold values from -6 to 6
- spread_up: float32 [3584, 14336], P('rows', 'tp'), may hold values from 0.1 to 10
- norm_gain: float32 [3584], P('rows'), may hold values from 0.25 to 1.75
Outputs:
- serving_gate: bfloat16 [3584, 14336], P(None, 'tp')
- serving_up: bfloat16 [3584, 14336], P(None, 'tp')
- column_gate: float32 [14336], P('tp')
- column_up: float32 [14336], P('tp')
The draws below stay inside these ranges and needn't reach their ends.
All inputs are finite; a program needn't handle non-finite values. Where the reference program divides by a largest or mean magnitude, that divisor is 1e-20 or more.
Results may differ from the reference program's by a relative error of at most 0.001.
Values may be sent and summed in bfloat16 or wider, within the bound.
A program may use at most 128 MiB of HBM per device.

```python
import math
import jax
import jax.numpy as jnp
from jax import lax

D_MODEL = 3584
D_INNER = 14336


def strengthened(values, rng, source, target, shards_of, factor):
    owner, partner = [(jnp.arange(values.shape[dim]) // (values.shape[dim] // shards_of)).reshape([-1 if axis == dim else 1 for axis in range(values.ndim)]) for dim in (source, target)]
    chosen = jax.random.permutation(rng, shards_of)[partner]
    strong = (owner == chosen) | (owner == (partner + shards_of // 2) % shards_of)
    return jnp.where(strong, factor * values, values)


def steps_of(own_key, shape, shards, low, high):
    def one(axis_at, parts):
        draws = jax.random.uniform(jax.random.fold_in(jax.random.fold_in(own_key, 6), axis_at), (parts,), jnp.float32, low / len(shards), high / len(shards))
        return jnp.repeat(jnp.exp(draws), shape[axis_at] // parts).reshape((-1,) + (1,) * (len(shape) - axis_at - 1))

    gain = one(*shards[0])
    for cut in shards[1:]:
        gain = gain * one(*cut)
    return gain


def bell_draw(own_key, shape, deviation, bound, split=(), dtype=jnp.bfloat16):
    gain = steps_of(own_key, shape, split, -0.22, 0.18) if split else 1.0
    drawn = jax.random.normal(own_key, shape, jnp.float32) * deviation * gain
    return jnp.minimum(jnp.maximum(drawn, -bound), bound).astype(dtype)


def gaussian_with(rng, extent, width, most, shards, heavy, held_as=jnp.bfloat16):
    drawn = width * jax.random.normal(rng, extent, jnp.float32)
    if shards:
        drawn = drawn * steps_of(rng, extent, shards, -0.22, 0.18)
    return jnp.clip(strengthened(drawn, jax.random.fold_in(rng, 3), *heavy), -most, most).astype(held_as)


def setup_inputs(seed: int = 0) -> dict:
    streams_of = jax.random.split(jax.random.key(seed), 8)
    return {
        "train_gate": gaussian_with(streams_of[0], (D_MODEL, D_INNER), D_MODEL ** -0.5, 0.125, ((0, 4), (1, 8)), (0, 1, 8, 2.0), jnp.float32),
        "drift_gate": bell_draw(streams_of[1], (D_MODEL, D_INNER), 1.0, 6.0, ((0, 4), (1, 8)), jnp.float32),
        "spread_gate": jnp.clip(jnp.exp(math.log(10.0) - 4.6051702 * jax.random.uniform(streams_of[2], (D_MODEL, D_INNER), jnp.float32) ** steps_of(streams_of[2], (D_MODEL, D_INNER), ((0, 4), (1, 8)), -0.2, 0.2)), 0.1, 10.0),
        "train_up": gaussian_with(streams_of[3], (D_MODEL, D_INNER), D_MODEL ** -0.5, 0.125, ((0, 4), (1, 8)), (0, 1, 8, 2.0), jnp.float32),
        "drift_up": bell_draw(streams_of[4], (D_MODEL, D_INNER), 1.0, 6.0, ((0, 4), (1, 8)), jnp.float32),
        "spread_up": jnp.clip(jnp.exp(math.log(10.0) - 4.6051702 * jax.random.uniform(streams_of[5], (D_MODEL, D_INNER), jnp.float32) ** steps_of(streams_of[5], (D_MODEL, D_INNER), ((0, 4), (1, 8)), -0.2, 0.2)), 0.1, 10.0),
        "norm_gain": jnp.clip(1.0 + 0.15 * jax.random.normal(streams_of[6], (D_MODEL,), jnp.float32), 0.25, 1.75),
    }


learn_rate = 0.015
decay_rate = 0.1
tiny_value = 1e-08

def reference(train_gate, drift_gate, spread_gate, train_up, drift_up, spread_up, norm_gain):
    whole_gate = train_gate - learn_rate * (drift_gate / (jnp.sqrt(spread_gate) + tiny_value) + decay_rate * train_gate)
    whole_up = train_up - learn_rate * (drift_up / (jnp.sqrt(spread_up) + tiny_value) + decay_rate * train_up)
    whole_gained_gate = whole_gate * norm_gain[:, None]
    whole_gained_up = whole_up * norm_gain[:, None]
    column_gate = lax.optimization_barrier(jnp.max(jnp.abs(whole_gained_gate), axis=0))
    serving_gate = (whole_gained_gate / column_gate).astype(jnp.bfloat16)
    column_up = lax.optimization_barrier(jnp.max(jnp.abs(whole_gained_up), axis=0))
    serving_up = (whole_gained_up / column_up).astype(jnp.bfloat16)
    return (serving_gate, serving_up, column_gate, column_up)
```

```python
import functools
import math

import jax
import jax.numpy as jnp
from jax import lax
from jax.experimental import pallas as pl
from jax.experimental.pallas import tpu as pltpu
from jax.sharding import PartitionSpec as P

learn_rate = 0.015
decay_rate = 0.1
tiny_value = 1e-08
MESH = pl.DeviceIdType.MESH
LANES = 128


def grid_of(rows):
    across = max(d for d in range(1, math.isqrt(rows) + 1) if rows % d == 0)
    return rows // across, across


def block_of(total, options):
    return next(b for b in options if total % b == 0)


def kernel(rows, width, step_rows, *refs):
    ins, gain, outs, columns = refs[:6], refs[6], refs[7:9], refs[9:11]
    stage, whole, peaks = refs[11:14]
    in_sem, peak_send, peak_recv, first_send, first_recv, next_send, next_recv = refs[14:]
    tall, wide = grid_of(rows)
    share, total = ins[0].shape
    chunks = total // width
    me = lax.axis_index("rows")
    my_y, my_x = me // wide, lax.rem(me, wide)

    def along_x(k):
        return my_y * wide + lax.rem(my_x + k, wide)

    def along_y(k):
        return lax.rem(my_y + k, tall) * wide + my_x

    plans = ((along_x, wide, along_y, tall), (along_y, tall, along_x, wide))

    def cols(c):
        return pl.ds(pl.multiple_of(c * width, LANES), width)

    def part(m, owner, c):
        return outs[m].at[pl.ds(pl.multiple_of(owner * share, step_rows), share), cols(c)]

    def load(c, slot):
        return [
            pltpu.make_async_copy(ins[a].at[:, cols(c)], stage.at[slot, a], in_sem.at[slot, a])
            for a in range(6)
        ]

    def send(ref, peer, send_sem, recv_sem):
        return pltpu.make_async_remote_copy(
            src_ref=ref, dst_ref=ref, send_sem=send_sem, recv_sem=recv_sem,
            device_id={"rows": peer}, device_id_type=MESH,
        )

    def peak_copy(c, k):
        return send(peaks.at[c, me], lax.rem(me + k, rows), peak_send.at[c, k], peak_recv.at[c, k])

    def peak_arrival(c, k):
        source = lax.rem(me + rows - k, rows)
        return send(peaks.at[c, source], source, peak_send.at[c, k], peak_recv.at[c, k])

    def first_copy(m, c, k, owner):
        return send(part(m, owner, c), plans[m][0](k), first_send.at[c, m, k], first_recv.at[c, m, k])

    def next_copy(m, c, j, k, owner):
        return send(part(m, owner, c), plans[m][2](k), next_send.at[c, m, j, k], next_recv.at[c, m, j, k])

    def owner_first(m, j):
        near, size = plans[m][:2]
        return near(size - j) if j else me

    def owner_next(m, j, k):
        y, x = my_y, my_x
        if m == 0:
            y, x = lax.rem(y + tall - k, tall), lax.rem(x + wide - j, wide)
        else:
            y, x = lax.rem(y + tall - j, tall), lax.rem(x + wide - k, wide)
        return y * wide + x

    for copy in load(0, 0):
        copy.start()

    @pl.when(chunks > 1)
    def _():
        for copy in load(min(1, chunks - 1), 1):
            copy.start()

    barrier = pltpu.get_barrier_semaphore()
    for k in range(1, rows):
        pl.semaphore_signal(
            barrier, inc=1, device_id={"rows": lax.rem(me + k, rows)}, device_id_type=MESH
        )
    pl.semaphore_wait(barrier, rows - 1)

    def update(c):
        slot = lax.rem(c, 2)
        for copy in load(c, slot):
            copy.wait()

        def step(i, most):
            at = pl.ds(pl.multiple_of(i * step_rows, step_rows), step_rows)
            g = gain[at, :]
            found = []
            for m in range(2):
                for t in range(width // LANES):
                    lane = pl.ds(t * LANES, LANES)
                    train, drift, spread = (stage[slot, 3 * m + a, at, lane] for a in range(3))
                    new = train - learn_rate * (
                        drift / (jnp.sqrt(spread) + tiny_value) + decay_rate * train
                    )
                    new = new * g
                    whole[slot, m, at, lane] = new
                    tops = jnp.max(jnp.abs(new).reshape(step_rows // 8, 8, LANES), axis=0)
                    found.append(jnp.maximum(most[len(found)], tops))
            return tuple(found)

        zero = jnp.zeros((8, LANES), jnp.float32)
        most = lax.fori_loop(0, share // step_rows, step, (zero,) * (2 * (width // LANES)))
        for m in range(2):
            for t in range(width // LANES):
                peaks[c, me, m : m + 1, pl.ds(t * LANES, LANES)] = jnp.max(
                    most[m * (width // LANES) + t], axis=0, keepdims=True
                )
        for k in range(1, rows):
            peak_copy(c, k).start()

    def finish(c):
        slot = lax.rem(c, 2)
        for k in range(1, rows):
            peak_arrival(c, k).wait_recv()
        scale = peaks[c, 0]
        for r in range(1, rows):
            scale = jnp.maximum(scale, peaks[c, r])
        for m in range(2):
            columns[m][:, cols(c)] = scale[m : m + 1, :]
        inverse = 1.0 / scale
        for m in range(2):
            factor = inverse[m : m + 1, :]

            def step(i, carry, m=m, factor=factor):
                at = pl.ds(pl.multiple_of(i * step_rows, step_rows), step_rows)
                to = pl.ds(pl.multiple_of(me * share + i * step_rows, step_rows), step_rows)
                outs[m][to, cols(c)] = (whole[slot, m, at, :] * factor).astype(jnp.bfloat16)
                return carry

            lax.fori_loop(0, share // step_rows, step, 0)
            for k in range(1, plans[m][1]):
                first_copy(m, c, k, me).start()

    update(0)

    def body(c, carry):
        @pl.when(c + 1 < chunks)
        def _():
            for copy in load(c + 1, lax.rem(c + 1, 2)):
                copy.start()

        update(c)
        finish(c - 1)
        return carry

    lax.fori_loop(1, chunks, body, 0)
    finish(chunks - 1)

    def own(c, carry):
        for m in range(2):
            for k in range(1, plans[m][3]):
                next_copy(m, c, 0, k, me).start()
        return carry

    lax.fori_loop(0, chunks, own, 0)

    def relay(c, carry):
        for j in range(1, max(tall, wide)):
            for m in range(2):
                if j < plans[m][1]:
                    first_copy(m, c, j, owner_first(m, j)).wait_recv()
                    for k in range(1, plans[m][3]):
                        next_copy(m, c, j, k, owner_first(m, j)).start()
        return carry

    lax.fori_loop(0, chunks, relay, 0)

    def drain(c, carry):
        for k in range(1, rows):
            peak_copy(c, k).wait_send()
        for m in range(2):
            for k in range(1, plans[m][1]):
                first_copy(m, c, k, me).wait_send()
            for j in range(plans[m][1]):
                for k in range(1, plans[m][3]):
                    next_copy(m, c, j, k, owner_first(m, j)).wait_send()
                    next_copy(m, c, j, k, owner_next(m, j, k)).wait_recv()
        return carry

    lax.fori_loop(0, chunks, drain, 0)


def settle(*arrays):
    pieces = 4

    def body(*refs):
        count = len(arrays)
        sem = refs[-1]
        copies = []
        for a in range(count):
            tall = arrays[a].shape[0] // pieces
            for p in range(pieces):
                at = pl.ds(p * tall, tall)
                copies.append(
                    pltpu.make_async_copy(refs[a].at[at], refs[count + a].at[at], sem.at[a, p])
                )
        for copy in copies:
            copy.start()
        for copy in copies:
            copy.wait()

    return pl.pallas_call(
        body,
        out_shape=tuple(jax.ShapeDtypeStruct(a.shape, a.dtype) for a in arrays),
        in_specs=[pl.BlockSpec(memory_space=pl.ANY)] * len(arrays),
        out_specs=(pl.BlockSpec(memory_space=pltpu.HBM),) * len(arrays),
        scratch_shapes=[pltpu.SemaphoreType.DMA((len(arrays), pieces))],
        compiler_params=pltpu.CompilerParams(vmem_limit_bytes=SMALL),
    )(*arrays)


def solution(mesh):
    rows = mesh.shape["rows"]

    def per_device(*args):
        arrays, norm_gain = args[:6], args[6]
        share, total = arrays[0].shape
        width = block_of(total, (256, LANES))
        step_rows = block_of(share, (32, 16))
        chunks = total // width
        most = max(grid_of(rows))
        gain = jnp.broadcast_to(norm_gain[:, None], (share, LANES))
        served = pltpu.VMEM((rows * share, total), jnp.bfloat16)
        column = pltpu.VMEM((1, total), jnp.float32)
        dma = pltpu.SemaphoreType.DMA
        serving_gate, serving_up, column_gate, column_up = pl.pallas_call(
            functools.partial(kernel, rows, width, step_rows),
            out_shape=OUT_SHAPES(served, column),
            in_specs=[pl.BlockSpec(memory_space=pltpu.HBM)] * 6
            + [pl.BlockSpec(memory_space=pltpu.VMEM)],
            out_specs=(pl.BlockSpec(memory_space=pltpu.VMEM),) * 4,
            scratch_shapes=[
                pltpu.VMEM((2, 6, share, width), jnp.float32),
                pltpu.VMEM((2, 2, share, width), jnp.float32),
                pltpu.VMEM((chunks, rows, 2, width), jnp.float32),
                dma((2, 6)),
                dma((chunks, rows)),
                dma((chunks, rows)),
                dma((chunks, 2, most)),
                dma((chunks, 2, most)),
                dma((chunks, 2, most, most)),
                dma((chunks, 2, most, most)),
            ],
            compiler_params=pltpu.CompilerParams(
                collective_id=0, has_side_effects=True, vmem_limit_bytes=VMEM_LIMIT
            ),
        )(*arrays, gain)
        serving_gate, serving_up = settle(serving_gate, serving_up)
        return serving_gate, serving_up, column_gate.reshape(total), column_up.reshape(total)

    split = P("rows", "tp")
    return jax.shard_map(
        per_device,
        mesh=mesh,
        in_specs=(split,) * 6 + (P("rows"),),
        out_specs=(P(None, "tp"), P(None, "tp"), P("tp"), P("tp")),
        check_vma=False,
    )


VMEM_LIMIT = 34 * 1024 * 1024
SMALL = 1024 * 1024


def OUT_SHAPES(served, column):
    return (served, served) + tuple(jax.ShapeDtypeStruct(r.shape, r.dtype) for r in (column, column))
```

```python
import functools
import math

import jax
import jax.numpy as jnp
from jax import lax
from jax.experimental import pallas as pl
from jax.experimental.pallas import tpu as pltpu
from jax.sharding import PartitionSpec as P

learn_rate = 0.015
decay_rate = 0.1
tiny_value = 1e-08
MESH = pl.DeviceIdType.MESH
LANES = 128


def grid_of(rows):
    across = max(d for d in range(1, math.isqrt(rows) + 1) if rows % d == 0)
    return rows // across, across


def block_of(total, options):
    return next(b for b in options if total % b == 0)


def kernel(rows, width, step_rows, *refs):
    ins, gains, outs, columns = refs[:6], refs[6], refs[7:9], refs[9:11]
    stage, whole, peaks, gain = refs[11:15]
    in_sem, peak_send, peak_recv, first_send, first_recv, next_send, next_recv = refs[15:]
    tall, wide = grid_of(rows)
    share, total = ins[0].shape
    chunks = total // width
    me = lax.axis_index("rows")
    my_y, my_x = me // wide, lax.rem(me, wide)

    def along_x(k):
        return my_y * wide + lax.rem(my_x + k, wide)

    def along_y(k):
        return lax.rem(my_y + k, tall) * wide + my_x

    plans = ((along_x, wide, along_y, tall), (along_y, tall, along_x, wide))

    def cols(c):
        return pl.ds(pl.multiple_of(c * width, LANES), width)

    def part(m, owner, c):
        return outs[m].at[pl.ds(pl.multiple_of(owner * share, step_rows), share), cols(c)]

    def load(c, slot):
        return [
            pltpu.make_async_copy(ins[a].at[:, cols(c)], stage.at[slot, a], in_sem.at[slot, a])
            for a in range(6)
        ]

    def send(ref, peer, send_sem, recv_sem):
        return pltpu.make_async_remote_copy(
            src_ref=ref, dst_ref=ref, send_sem=send_sem, recv_sem=recv_sem,
            device_id={"rows": peer}, device_id_type=MESH,
        )

    def peak_copy(c, k):
        return send(peaks.at[c, me], lax.rem(me + k, rows), peak_send.at[c, k], peak_recv.at[c, k])

    def peak_arrival(c, k):
        source = lax.rem(me + rows - k, rows)
        return send(peaks.at[c, source], source, peak_send.at[c, k], peak_recv.at[c, k])

    def first_copy(m, c, k, owner):
        return send(part(m, owner, c), plans[m][0](k), first_send.at[c, m, k], first_recv.at[c, m, k])

    def next_copy(m, c, j, k, owner):
        return send(part(m, owner, c), plans[m][2](k), next_send.at[c, m, j, k], next_recv.at[c, m, j, k])

    def owner_first(m, j):
        near, size = plans[m][:2]
        return near(size - j) if j else me

    def owner_next(m, j, k):
        y, x = my_y, my_x
        if m == 0:
            y, x = lax.rem(y + tall - k, tall), lax.rem(x + wide - j, wide)
        else:
            y, x = lax.rem(y + tall - j, tall), lax.rem(x + wide - k, wide)
        return y * wide + x

    for copy in load(0, 0):
        copy.start()

    @pl.when(chunks > 1)
    def _():
        for copy in load(min(1, chunks - 1), 1):
            copy.start()

    barrier = pltpu.get_barrier_semaphore()
    for k in range(1, rows):
        pl.semaphore_signal(
            barrier, inc=1, device_id={"rows": lax.rem(me + k, rows)}, device_id_type=MESH
        )
    pl.semaphore_wait(barrier, rows - 1)

    for start in range(0, share, LANES):
        count = min(LANES, share - start)
        line = gains[pl.ds(start, count)].reshape(1, count)
        gain[pl.ds(start, count), :] = jnp.broadcast_to(line, (LANES, count)).T

    def update(c):
        slot = lax.rem(c, 2)
        for copy in load(c, slot):
            copy.wait()

        def step(i, most):
            at = pl.ds(pl.multiple_of(i * step_rows, step_rows), step_rows)
            g = gain[at, :]
            found = []
            for m in range(2):
                for t in range(width // LANES):
                    lane = pl.ds(t * LANES, LANES)
                    train, drift, spread = (stage[slot, 3 * m + a, at, lane] for a in range(3))
                    new = train - learn_rate * (
                        drift / (jnp.sqrt(spread) + tiny_value) + decay_rate * train
                    )
                    new = new * g
                    whole[slot, m, at, lane] = new
                    tops = jnp.max(jnp.abs(new).reshape(step_rows // 8, 8, LANES), axis=0)
                    found.append(jnp.maximum(most[len(found)], tops))
            return tuple(found)

        zero = jnp.zeros((8, LANES), jnp.float32)
        most = lax.fori_loop(0, share // step_rows, step, (zero,) * (2 * (width // LANES)))
        for m in range(2):
            for t in range(width // LANES):
                peaks[c, me, m : m + 1, pl.ds(t * LANES, LANES)] = jnp.max(
                    most[m * (width // LANES) + t], axis=0, keepdims=True
                )
        for k in range(1, rows):
            peak_copy(c, k).start()

    def finish(c):
        slot = lax.rem(c, 2)
        for k in range(1, rows):
            peak_arrival(c, k).wait_recv()
        scale = peaks[c, 0]
        for r in range(1, rows):
            scale = jnp.maximum(scale, peaks[c, r])
        for m in range(2):
            columns[m][cols(c)] = scale[m]
        inverse = 1.0 / scale
        for m in range(2):
            factor = inverse[m : m + 1, :]

            def step(i, carry, m=m, factor=factor):
                at = pl.ds(pl.multiple_of(i * step_rows, step_rows), step_rows)
                to = pl.ds(pl.multiple_of(me * share + i * step_rows, step_rows), step_rows)
                outs[m][to, cols(c)] = (whole[slot, m, at, :] * factor).astype(jnp.bfloat16)
                return carry

            lax.fori_loop(0, share // step_rows, step, 0)
            for k in range(1, plans[m][1]):
                first_copy(m, c, k, me).start()

    update(0)

    def body(c, carry):
        @pl.when(c + 1 < chunks)
        def _():
            for copy in load(c + 1, lax.rem(c + 1, 2)):
                copy.start()

        update(c)
        finish(c - 1)
        return carry

    lax.fori_loop(1, chunks, body, 0)
    finish(chunks - 1)

    def own(c, carry):
        for m in range(2):
            for k in range(1, plans[m][3]):
                next_copy(m, c, 0, k, me).start()
        return carry

    lax.fori_loop(0, chunks, own, 0)

    def relay(c, carry):
        for j in range(1, max(tall, wide)):
            for m in range(2):
                if j < plans[m][1]:
                    first_copy(m, c, j, owner_first(m, j)).wait_recv()
                    for k in range(1, plans[m][3]):
                        next_copy(m, c, j, k, owner_first(m, j)).start()
        return carry

    lax.fori_loop(0, chunks, relay, 0)

    def drain(c, carry):
        for k in range(1, rows):
            peak_copy(c, k).wait_send()
        for m in range(2):
            for k in range(1, plans[m][1]):
                first_copy(m, c, k, me).wait_send()
            for j in range(plans[m][1]):
                for k in range(1, plans[m][3]):
                    next_copy(m, c, j, k, owner_first(m, j)).wait_send()
                    next_copy(m, c, j, k, owner_next(m, j, k)).wait_recv()
        return carry

    lax.fori_loop(0, chunks, drain, 0)


def settle(pieces, *arrays):
    def body(*refs):
        count = len(arrays)
        sem = refs[-1]
        copies = []
        for a in range(count):
            parts = pieces if arrays[a].ndim > 1 else 1
            tall = arrays[a].shape[0] // parts
            for p in range(parts):
                at = pl.ds(p * tall, tall)
                copies.append(
                    pltpu.make_async_copy(refs[a].at[at], refs[count + a].at[at], sem.at[a, p])
                )
        for copy in copies:
            copy.start()
        for copy in copies:
            copy.wait()

    return pl.pallas_call(
        body,
        out_shape=tuple(jax.ShapeDtypeStruct(a.shape, a.dtype) for a in arrays),
        in_specs=[pl.BlockSpec(memory_space=pl.ANY)] * len(arrays),
        out_specs=(pl.BlockSpec(memory_space=pltpu.HBM),) * len(arrays),
        scratch_shapes=[pltpu.SemaphoreType.DMA((len(arrays), pieces))],
        compiler_params=pltpu.CompilerParams(vmem_limit_bytes=SMALL),
    )(*arrays)


def solution(mesh):
    rows = mesh.shape["rows"]

    def per_device(*args):
        arrays, norm_gain = args[:6], args[6]
        share, total = arrays[0].shape
        width = block_of(total, (LANES,))
        step_rows = block_of(share, (32, 16))
        chunks = total // width
        most = max(grid_of(rows))
        served = pltpu.VMEM((rows * share, total), jnp.bfloat16)
        column = pltpu.VMEM((total,), jnp.float32)
        dma = pltpu.SemaphoreType.DMA
        serving_gate, serving_up, column_gate, column_up = pl.pallas_call(
            functools.partial(kernel, rows, width, step_rows),
            out_shape=(served, served, column, column),
            in_specs=[pl.BlockSpec(memory_space=pltpu.HBM)] * 6
            + [pl.BlockSpec(memory_space=pltpu.VMEM)],
            out_specs=(pl.BlockSpec(memory_space=pltpu.VMEM),) * 4,
            scratch_shapes=[
                pltpu.VMEM((2, 6, share, width), jnp.float32),
                pltpu.VMEM((2, 2, share, width), jnp.float32),
                pltpu.VMEM((chunks, rows, 2, width), jnp.float32),
                pltpu.VMEM((share, LANES), jnp.float32),
                dma((2, 6)),
                dma((chunks, rows)),
                dma((chunks, rows)),
                dma((chunks, 2, most)),
                dma((chunks, 2, most)),
                dma((chunks, 2, most, most)),
                dma((chunks, 2, most, most)),
            ],
            compiler_params=pltpu.CompilerParams(
                collective_id=0, has_side_effects=True, vmem_limit_bytes=VMEM_LIMIT
            ),
        )(*arrays, norm_gain)
        return settle(2 * rows, serving_gate, serving_up, column_gate, column_up)

    split = P("rows", "tp")
    return jax.shard_map(
        per_device,
        mesh=mesh,
        in_specs=(split,) * 6 + (P("rows"),),
        out_specs=(P(None, "tp"), P(None, "tp"), P("tp"), P("tp")),
        check_vma=False,
    )


VMEM_LIMIT = 34 * 1024 * 1024
SMALL = 1024 * 1024
```
